8 devices in a mesh: fsdp: 8 (over z, y, x, core).
Axes of the slice: x: 2, y: 2, z: 1, core: 2. Of those that a mesh axis runs over, the one named last changes fastest.
Arguments:
- tokens_x: bfloat16 [48, 256, 640], P('fsdp')
- context: bfloat16 [48, 77, 1024], P('fsdp')
- cot_out: bfloat16 [48, 256, 640], P('fsdp')
- w_qkv: bfloat16 [2, 1228800], P(None, 'fsdp')
- w_out: bfloat16 [2, 409600], P(None, 'fsdp')
- w_q2: bfloat16 [2, 409600], P(None, 'fsdp')
- w_kv2: bfloat16 [2, 1310720], P(None, 'fsdp')
- w_out2: bfloat16 [2, 409600], P(None, 'fsdp')
- w_ff1: bfloat16 [2, 3276800], P(None, 'fsdp')
- w_ff2: bfloat16 [2, 1638400], P(None, 'fsdp')
- w_vecs: bfloat16 [2, 10880], P(None, 'fsdp')
Outputs:
- output 1: bfloat16 [48, 256, 640], P('fsdp')
- output 2: bfloat16 [48, 256, 640], P('fsdp')
- output 3: float32 [2, 1228800], P(None, 'fsdp')
- output 4: float32 [2, 409600], P(None, 'fsdp')
- output 5: float32 [2, 409600], P(None, 'fsdp')
- output 6: float32 [2, 1310720], P(None, 'fsdp')
- output 7: float32 [2, 409600], P(None, 'fsdp')
- output 8: float32 [2, 3276800], P(None, 'fsdp')
- output 9: float32 [2, 1638400], P(None, 'fsdp')
- output 10: float32 [2, 10880], P(None, 'fsdp')
All inputs are finite; a program needn't handle non-finite values.
Results may differ from the reference program's by a relative error of at most 0.01997.
Values are sent between devices in bfloat16 or wider.
A program may use at most 1 GiB of HBM per device.

```python
import math
import jax
import jax.numpy as jnp
from jax import lax

FSDP = 8
BATCH_DEV = 6
TOKENS = 256
D = 640
CTX_D = 1024
CTX_LEN = 77
HEAD = 64
BLOCKS = 2

BATCH = FSDP * BATCH_DEV
HEADS = D // HEAD
FF = 4 * D
SHAPES = ((D, 3 * D), (D, D), (D, D), (CTX_D, 2 * D), (D, D), (D, 2 * FF), (FF, D), (9 * D + 2 * FF,))
NAMES = ('w_qkv', 'w_out', 'w_q2', 'w_kv2', 'w_out2', 'w_ff1', 'w_ff2', 'w_vecs')


def padded_len(shape):
    return ((math.prod(shape) + FSDP - 1) // FSDP) * FSDP


def setup_inputs(seed: int = 0) -> dict:
    draws = jax.random.split(jax.random.key(seed), 11)
    tokens_x = jax.random.normal(draws[0], (BATCH, TOKENS, D), jnp.float32)
    context = jax.random.normal(draws[1], (BATCH, CTX_LEN, CTX_D), jnp.float32)
    cot_out = jax.random.normal(draws[2], (BATCH, TOKENS, D), jnp.float32)
    result = {'tokens_x': tokens_x.astype(jnp.bfloat16), 'context': context.astype(jnp.bfloat16), 'cot_out': cot_out.astype(jnp.bfloat16)}
    for index in range(7):
        shape = SHAPES[index]
        drawn = jax.random.normal(draws[3 + index], (BLOCKS, padded_len(shape)), jnp.float32) * shape[0] ** -0.5
        result[NAMES[index]] = drawn.astype(jnp.bfloat16)
    length = padded_len(SHAPES[7])
    position = jnp.arange(length)
    gain_mask = ((position < 6 * D) & ((position // D) % 2 == 0)).astype(jnp.float32)
    drawn = 0.3 * jax.random.normal(draws[10], (BLOCKS, length), jnp.float32) + gain_mask
    result['w_vecs'] = drawn.astype(jnp.bfloat16)
    return result


def matmul(lhs, rhs):
    return jnp.dot(lhs, rhs, preferred_element_type=jnp.float32)


def layer_norm(residual, gain, shift):
    average = jnp.mean(residual, axis=-1, keepdims=True)
    centered = residual - average
    variance = jnp.mean(centered * centered, axis=-1, keepdims=True)
    return centered * lax.rsqrt(variance + 1e-5) * gain + shift


def attend(query, keys, values):
    scores = jnp.einsum('qhe,khe->hqk', query.astype(jnp.float32), keys.astype(jnp.float32)) * HEAD ** -0.5
    probabilities = jax.nn.softmax(scores, axis=-1).astype(jnp.bfloat16)
    mixed = jnp.einsum('hqk,khe->qhe', probabilities.astype(jnp.float32), values.astype(jnp.float32))
    return mixed.astype(jnp.bfloat16)


def batched_attend(query, keys, values):
    return lax.map(lambda trio: attend(trio[0], trio[1], trio[2]), (query, keys, values))


def block_forward(residual, ctx_rows, flats):
    matrices = [flat[:math.prod(shape)].reshape(shape).astype(jnp.bfloat16) for flat, shape in zip(flats[:7], SHAPES[:7])]
    w_qkv, w_out, w_q2, w_kv2, w_out2, w_ff1, w_ff2 = matrices
    rows = flats[7][:9 * D].reshape(9, D)
    bias_ff1 = flats[7][9 * D:9 * D + 2 * FF]
    norm1 = layer_norm(residual, rows[0], rows[1]).astype(jnp.bfloat16)
    qkv_heads = matmul(norm1, w_qkv).astype(jnp.bfloat16).reshape(BATCH, TOKENS, 3, HEADS, HEAD)
    self_out = batched_attend(qkv_heads[:, :, 0], qkv_heads[:, :, 1], qkv_heads[:, :, 2]).reshape(BATCH * TOKENS, D)
    residual = residual + matmul(self_out, w_out) + rows[6]
    norm2 = layer_norm(residual, rows[2], rows[3]).astype(jnp.bfloat16)
    query = matmul(norm2, w_q2).astype(jnp.bfloat16).reshape(BATCH, TOKENS, HEADS, HEAD)
    kv_heads = matmul(ctx_rows, w_kv2).astype(jnp.bfloat16).reshape(BATCH, CTX_LEN, 2, HEADS, HEAD)
    cross_out = batched_attend(query, kv_heads[:, :, 0], kv_heads[:, :, 1]).reshape(BATCH * TOKENS, D)
    residual = residual + matmul(cross_out, w_out2) + rows[7]
    norm3 = layer_norm(residual, rows[4], rows[5]).astype(jnp.bfloat16)
    hidden = matmul(norm3, w_ff1) + bias_ff1
    gated = (hidden[:, :FF] * jax.nn.gelu(hidden[:, FF:], approximate=False)).astype(jnp.bfloat16)
    return residual + matmul(gated, w_ff2) + rows[8]


def forward(tokens_x, context, flats):
    residual = tokens_x.reshape(BATCH * TOKENS, D).astype(jnp.float32)
    ctx_rows = context.reshape(BATCH * CTX_LEN, CTX_D)

    def step(carry, block_flats):
        return block_forward(carry, ctx_rows, block_flats), None

    residual, unused = lax.scan(step, residual, flats)
    return residual.astype(jnp.bfloat16).reshape(BATCH, TOKENS, D)


def reference(tokens_x, context, cot_out, w_qkv, w_out, w_q2, w_kv2, w_out2, w_ff1, w_ff2, w_vecs):
    flats = tuple(param.astype(jnp.float32) for param in (w_qkv, w_out, w_q2, w_kv2, w_out2, w_ff1, w_ff2, w_vecs))
    out_tokens, pullback = jax.vjp(lambda tok_in, param_set: forward(tok_in, context, param_set), tokens_x, flats)
    grad_x, grads = pullback(cot_out)
    scaled = [grad_item / BATCH for grad_item in grads]
    return (out_tokens, grad_x, scaled[0], scaled[1], scaled[2], scaled[3], scaled[4], scaled[5], scaled[6], scaled[7])
```

```python
import math
import jax
import jax.numpy as jnp
from jax import lax
from jax.experimental import pallas as pl
from jax.experimental.pallas import tpu as pltpu
from jax.sharding import PartitionSpec as P

HEAD = 64
AXIS = 'fsdp'


def weight_shapes(width, ctx_width):
    return ((width, 3 * width), (width, width), (width, width), (ctx_width, 2 * width),
            (width, width), (width, 8 * width), (4 * width, width), (17 * width,))


def layer_norm(residual, gain, shift):
    average = jnp.mean(residual, axis=-1, keepdims=True)
    centered = residual - average
    variance = jnp.mean(centered * centered, axis=-1, keepdims=True)
    return centered * lax.rsqrt(variance + 1e-5) * gain + shift


def dot_nt(lhs, rhs):
    return lax.dot_general(lhs, rhs, (((1,), (1,)), ((), ())), preferred_element_type=jnp.float32)


def dot_tn(lhs, rhs):
    return lax.dot_general(lhs, rhs, (((0,), (0,)), ((), ())), preferred_element_type=jnp.float32)


def dot_nn(lhs, rhs):
    return lax.dot_general(lhs, rhs, (((1,), (0,)), ((), ())), preferred_element_type=jnp.float32)


def head_probs(query, keys, n_keys):
    scores = dot_nt(query, keys) * HEAD ** -0.5
    if n_keys < keys.shape[0]:
        column = lax.broadcasted_iota(jnp.int32, scores.shape, 1)
        scores = jnp.where(column < n_keys, scores, -jnp.inf)
    weight = jnp.exp(scores - jnp.max(scores, axis=1, keepdims=True))
    return weight / jnp.sum(weight, axis=1, keepdims=True)


def head_back(query, keys, values, d_out, n_keys):
    probs = head_probs(query, keys, n_keys)
    d_values = dot_tn(probs.astype(jnp.bfloat16), d_out)
    d_probs = dot_nt(d_out, values)
    inner = jnp.sum(probs * d_probs, axis=1, keepdims=True)
    d_scores = (probs * (d_probs - inner) * HEAD ** -0.5).astype(jnp.bfloat16)
    return dot_nn(d_scores, keys), dot_tn(d_scores, query), d_values


def lanes(start):
    return slice(start, start + HEAD)


def attend_kernel(width, n_keys, q_ref, kv_ref, k_at, v_at, out_ref):
    for pair in range(width // (2 * HEAD)):
        mixed = []
        for at in (2 * pair * HEAD, (2 * pair + 1) * HEAD):
            probs = head_probs(q_ref[0, :, lanes(at)], kv_ref[0, :, lanes(k_at + at)], n_keys)
            mixed.append(dot_nn(probs.astype(jnp.bfloat16), kv_ref[0, :, lanes(v_at + at)]))
        both = jnp.concatenate(mixed, axis=1).astype(jnp.bfloat16)
        out_ref[0, :, 2 * pair * HEAD:2 * (pair + 1) * HEAD] = both


def attend_back_kernel(width, n_keys, q_ref, kv_ref, k_at, v_at, d_ref, dq_ref, dkv_ref):
    for pair in range(width // (2 * HEAD)):
        grads = []
        for at in (2 * pair * HEAD, (2 * pair + 1) * HEAD):
            grads.append(head_back(q_ref[0, :, lanes(at)], kv_ref[0, :, lanes(k_at + at)],
                                   kv_ref[0, :, lanes(v_at + at)], d_ref[0, :, lanes(at)], n_keys))
        dq, dk, dv = [jnp.concatenate(two, axis=1).astype(jnp.bfloat16) for two in zip(*grads)]
        at = 2 * pair * HEAD
        dq_ref[0, :, at:at + 2 * HEAD] = dq
        dkv_ref[0, :, k_at + at:k_at + at + 2 * HEAD] = dk
        dkv_ref[0, :, v_at + at:v_at + at + 2 * HEAD] = dv


def sample_spec(array):
    return pl.BlockSpec((1,) + array.shape[1:], lambda index: (index, 0, 0))


def per_sample(body, inputs, outputs, flops):
    moved = sum(array.size * array.dtype.itemsize for array in list(inputs) + list(outputs))
    return pl.pallas_call(
        body, grid=(inputs[0].shape[0],),
        in_specs=[sample_spec(array) for array in inputs],
        out_specs=[sample_spec(array) for array in outputs],
        out_shape=list(outputs),
        compiler_params=pltpu.CompilerParams(dimension_semantics=('arbitrary',), vmem_limit_bytes=48 * 1024 * 1024),
        cost_estimate=pl.CostEstimate(flops=flops, bytes_accessed=moved, transcendentals=0),
    )(*inputs)


def shaped(array, last=None, dtype=None):
    shape = array.shape if last is None else array.shape[:-1] + (last,)
    return jax.ShapeDtypeStruct(shape, dtype or array.dtype)


def self_attend(qkv):
    width = qkv.shape[-1] // 3
    tokens = qkv.shape[1]

    def body(qkv_ref, out_ref):
        attend_kernel(width, tokens, qkv_ref, qkv_ref, width, 2 * width, out_ref)

    return per_sample(body, [qkv], [shaped(qkv, width)], 8 * qkv.shape[0] * tokens * tokens * width)[0]


def self_attend_back(qkv, d_out):
    width = d_out.shape[-1]
    tokens = qkv.shape[1]

    def body(qkv_ref, d_ref, dqkv_ref):
        attend_back_kernel(width, tokens, qkv_ref, qkv_ref, width, 2 * width, d_ref, dqkv_ref, dqkv_ref)

    return per_sample(body, [qkv, d_out], [shaped(qkv)], 20 * qkv.shape[0] * tokens * tokens * width)[0]


def cross_attend(query, keys_values, n_keys):
    width = query.shape[-1]

    def body(q_ref, kv_ref, out_ref):
        attend_kernel(width, n_keys, q_ref, kv_ref, 0, width, out_ref)

    flops = 8 * query.shape[0] * query.shape[1] * keys_values.shape[1] * width
    return per_sample(body, [query, keys_values], [shaped(query)], flops)[0]


def cross_attend_back(query, keys_values, d_out, n_keys):
    width = query.shape[-1]

    def body(q_ref, kv_ref, d_ref, dq_ref, dkv_ref):
        attend_back_kernel(width, n_keys, q_ref, kv_ref, 0, width, d_ref, dq_ref, dkv_ref)

    flops = 20 * query.shape[0] * query.shape[1] * keys_values.shape[1] * width
    return per_sample(body, [query, keys_values, d_out], [shaped(query), shaped(keys_values)], flops)


FF_TILE = 512
ROW_TILE = 256


def normal_cdf(value):
    return 0.5 * (1.0 + lax.erf(value * (0.5 ** 0.5)))


def ff_forward(norm, w_ff1, bias, w_ff2):
    rows, width = norm.shape
    half = w_ff2.shape[0]

    def body(norm_ref, w1_ref, bias_ref, w2_ref, out_ref):
        total = jnp.zeros((ROW_TILE, width), jnp.float32)
        for start in range(0, half, FF_TILE):
            side_a, side_g = slice(start, start + FF_TILE), slice(half + start, half + start + FF_TILE)
            u_a = dot_nn(norm_ref[...], w1_ref[:, side_a]) + bias_ref[:, side_a]
            u_g = dot_nn(norm_ref[...], w1_ref[:, side_g]) + bias_ref[:, side_g]
            gated = (u_a * (u_g * normal_cdf(u_g))).astype(jnp.bfloat16)
            total = total + dot_nn(gated, w2_ref[side_a, :])
        out_ref[...] = total

    whole = lambda index: (0, 0)
    return pl.pallas_call(
        body, grid=(rows // ROW_TILE,),
        in_specs=[pl.BlockSpec((ROW_TILE, width), lambda index: (index, 0)), pl.BlockSpec(w_ff1.shape, whole),
                  pl.BlockSpec(bias.shape, whole), pl.BlockSpec(w_ff2.shape, whole)],
        out_specs=pl.BlockSpec((ROW_TILE, width), lambda index: (index, 0)),
        out_shape=jax.ShapeDtypeStruct((rows, width), jnp.float32),
        compiler_params=pltpu.CompilerParams(dimension_semantics=('arbitrary',), vmem_limit_bytes=56 * 1024 * 1024),
        cost_estimate=pl.CostEstimate(flops=6 * rows * width * half, bytes_accessed=20_000_000, transcendentals=0),
    )(norm, w_ff1, bias, w_ff2)


def ff_backward(norm, grad_bf, w_ff1, bias, w_ff2):
    rows, width = norm.shape
    half = w_ff2.shape[0]
    tiles = half // FF_TILE

    def body(norm_ref, grad_ref, w1a_ref, w1g_ref, ba_ref, bg_ref, w2_ref,
             dw1_ref, dw2_ref, db_ref, dnorm_ref, z_ref, da_ref, dg_ref, acc_ref):
        step = pl.program_id(0)
        acc_ref[...] = jnp.zeros_like(acc_ref)

        @pl.when(step == 0)
        def _():
            dnorm_ref[...] = jnp.zeros_like(dnorm_ref)

        def tile(index, carry):
            here = pl.ds(pl.multiple_of(index * ROW_TILE, ROW_TILE), ROW_TILE)
            norm_tile = norm_ref[here, :]
            u_a = dot_nn(norm_tile, w1a_ref[...]) + ba_ref[...]
            u_g = dot_nn(norm_tile, w1g_ref[...]) + bg_ref[...]
            d_gated = dot_nt(grad_ref[here, :], w2_ref[...]).astype(jnp.bfloat16).astype(jnp.float32)
            cdf = normal_cdf(u_g)
            gate = u_g * cdf
            slope = cdf + u_g * (jnp.exp(-0.5 * u_g * u_g) * ((2.0 * math.pi) ** -0.5))
            z_ref[here, :] = (u_a * gate).astype(jnp.bfloat16)
            d_a = d_gated * gate
            d_g = d_gated * u_a * slope
            acc_ref[0:1, :] += jnp.sum(d_a, axis=0, keepdims=True)
            acc_ref[1:2, :] += jnp.sum(d_g, axis=0, keepdims=True)
            d_a, d_g = d_a.astype(jnp.bfloat16), d_g.astype(jnp.bfloat16)
            da_ref[here, :] = d_a
            dg_ref[here, :] = d_g
            dnorm_ref[here, :] += dot_nt(d_a, w1a_ref[...]) + dot_nt(d_g, w1g_ref[...])
            return carry

        lax.fori_loop(0, rows // ROW_TILE, tile, 0)
        dw1_ref[0] = dot_tn(norm_ref[...], da_ref[...]).astype(jnp.bfloat16)
        dw1_ref[1] = dot_tn(norm_ref[...], dg_ref[...]).astype(jnp.bfloat16)
        dw2_ref[...] = dot_tn(z_ref[...], grad_ref[...]).astype(jnp.bfloat16)
        db_ref[...] = acc_ref[0:2, :]

    whole = lambda index: (0, 0)
    return pl.pallas_call(
        body, grid=(tiles,),
        in_specs=[pl.BlockSpec((rows, width), whole), pl.BlockSpec((rows, width), whole),
                  pl.BlockSpec((width, FF_TILE), lambda index: (0, index)),
                  pl.BlockSpec((width, FF_TILE), lambda index: (0, index + tiles)),
                  pl.BlockSpec((1, FF_TILE), lambda index: (0, index)),
                  pl.BlockSpec((1, FF_TILE), lambda index: (0, index + tiles)),
                  pl.BlockSpec((FF_TILE, width), lambda index: (index, 0))],
        out_specs=[pl.BlockSpec((2, width, FF_TILE), lambda index: (0, 0, index)),
                   pl.BlockSpec((FF_TILE, width), lambda index: (index, 0)),
                   pl.BlockSpec((2, FF_TILE), lambda index: (0, index)),
                   pl.BlockSpec((rows, width), whole)],
        out_shape=[jax.ShapeDtypeStruct((2, width, half), jnp.bfloat16),
                   jax.ShapeDtypeStruct((half, width), jnp.bfloat16),
                   jax.ShapeDtypeStruct((2, half), jnp.float32),
                   jax.ShapeDtypeStruct((rows, width), jnp.float32)],
        scratch_shapes=[pltpu.VMEM((rows, FF_TILE), jnp.bfloat16), pltpu.VMEM((rows, FF_TILE), jnp.bfloat16),
                        pltpu.VMEM((rows, FF_TILE), jnp.bfloat16), pltpu.VMEM((8, FF_TILE), jnp.float32)],
        compiler_params=pltpu.CompilerParams(dimension_semantics=('arbitrary',), vmem_limit_bytes=56 * 1024 * 1024),
        cost_estimate=pl.CostEstimate(flops=16 * rows * width * half, bytes_accessed=40_000_000, transcendentals=0),
    )(norm, grad_bf, w_ff1, w_ff1, bias, bias, w_ff2)


def project(inputs, weight):
    return jnp.einsum('btd,de->bte', inputs, weight, preferred_element_type=jnp.float32)


def project_back(grads, weight):
    return jnp.einsum('bte,de->btd', grads, weight, preferred_element_type=jnp.float32)


def weight_grad(inputs, grads):
    return jnp.einsum('btd,bte->de', inputs, grads, preferred_element_type=jnp.float32)


def swap(value, bit):
    return lax.ppermute(value, AXIS, [(index, index ^ bit) for index in range(8)])


def coords():
    me = lax.axis_index(AXIS)
    return (me >> 2) & 1, (me >> 1) & 1, me & 1


def join(mine, other, bit, axis):
    low = jnp.where(bit == 0, mine, other)
    high = jnp.where(bit == 0, other, mine)
    return jnp.stack([low, high], axis=axis)


class Task:
    def __init__(self, steps):
        self.steps = steps
        self.pending = next(steps)
        self.result = None

    def advance(self, value):
        try:
            self.pending = self.steps.send(value)
        except StopIteration as stop:
            self.pending = None
            self.result = stop.value


def tick(chain, tasks):
    live = [task for task in tasks if task.pending is not None]
    if not live:
        return chain
    chain, values = lax.optimization_barrier((chain, [task.pending for task in live]))
    for task, value in zip(live, values):
        task.advance(value)
    return chain


def drain(tasks):
    while any(task.pending is not None for task in tasks):
        for task in tasks:
            if task.pending is not None:
                task.advance(task.pending)


def gather_steps(piece, x_first):
    y_bit, x_bit, core = coords()
    shape = (8 * piece.shape[0], piece.shape[1])
    piece = yield piece
    if x_first:
        other = yield swap(piece, 2)
        held = join(piece, other, x_bit, 0)
        other = yield swap(held, 4)
        held = join(held, other, y_bit, 0)
    else:
        other = yield swap(piece, 4)
        held = join(piece, other, y_bit, 0)
        other = yield swap(held, 2)
        held = join(held, other, x_bit, 1)
    other = yield swap(held, 1)
    return join(held, other, core, 2).reshape(shape)


def keep_and_send(value, bit, axis):
    keep = lax.dynamic_index_in_dim(value, bit, axis, keepdims=False)
    send = lax.dynamic_index_in_dim(value, 1 - bit, axis, keepdims=False)
    return keep, send


def scatter_steps(partial, x_first):
    y_bit, x_bit, core = coords()
    partial = yield partial
    lead = partial.ndim - 3
    held = partial.reshape(partial.shape[:lead] + (2, 2, 2) + partial.shape[lead + 1:])
    hops = [(core, 2, 1)] + ([(x_bit, 1, 2), (y_bit, 0, 4)] if x_first else [(y_bit, 0, 4), (x_bit, 1, 2)])
    for number, (coord, axis, bit) in enumerate(hops):
        if number == 2:
            axis = 0
        keep, send = keep_and_send(held, coord, axis + lead)
        other = yield swap(send, bit)
        held = keep.astype(jnp.float32) + other.astype(jnp.float32)
        if number < 2:
            held = held.astype(jnp.bfloat16)
    return held


VEC_ROWS = 8


def vec_to_rows(flat, width):
    return jnp.pad(flat, (0, VEC_ROWS * width - flat.shape[0])).reshape(VEC_ROWS, width)


def gather_tasks(shards, width, ctx_width, layer):
    shapes = weight_shapes(width, ctx_width)
    flip = layer % 2 == 1
    two_d = [shard.reshape(shape[0] // 8, shape[1]) for shard, shape in zip(shards[:7], shapes[:7])]
    square = jnp.concatenate([two_d[1], two_d[2], two_d[4], vec_to_rows(shards[7], width)], axis=0)
    return dict(qkv=Task(gather_steps(two_d[0], not flip)), square=Task(gather_steps(square, flip)),
                kv2=Task(gather_steps(two_d[3], flip)), ff1=Task(gather_steps(two_d[5], not flip)),
                ff2=Task(gather_steps(two_d[6], flip)))


def square_weights(tasks, width, shard_len):
    rows = width // 8
    squares = tasks['square'].result.reshape(8, -1, width)
    parts = [squares[:, index * rows:(index + 1) * rows].reshape(width, width) for index in range(3)]
    vec_flat = squares[:, 3 * rows:].reshape(8, -1)[:, :shard_len].reshape(-1)
    return dict(w_out=parts[0], w_q2=parts[1], w_out2=parts[2],
                rows=vec_flat[:9 * width].reshape(9, width).astype(jnp.float32),
                bias_ff1=vec_flat[9 * width:17 * width].astype(jnp.float32))


def block_forward(residual, context, n_keys, tasks, shard_len, pace):
    batch, tokens, width = residual.shape
    weights = square_weights(tasks, width, shard_len)
    weights['w_qkv'] = tasks['qkv'].result
    rows = weights['rows']
    norm1, ln1_back = jax.vjp(layer_norm, residual, rows[0], rows[1])
    norm1 = norm1.astype(jnp.bfloat16)
    qkv = project(norm1, weights['w_qkv']).astype(jnp.bfloat16)
    qkv = pace(0, qkv)
    self_out = pace(1, self_attend(qkv))
    residual = residual + project(self_out, weights['w_out']) + rows[6]
    norm2, ln2_back = jax.vjp(layer_norm, residual, rows[2], rows[3])
    norm2 = norm2.astype(jnp.bfloat16)
    query = project(norm2, weights['w_q2']).astype(jnp.bfloat16)
    query = pace(2, query)
    weights['w_kv2'] = tasks['kv2'].result
    keys_values = project(context, weights['w_kv2']).astype(jnp.bfloat16)
    cross_out = pace(3, cross_attend(query, keys_values, n_keys))
    weights['w_ff1'], weights['w_ff2'] = tasks['ff1'].result, tasks['ff2'].result
    residual = residual + project(cross_out, weights['w_out2']) + rows[7]
    norm3, ln3_back = jax.vjp(layer_norm, residual, rows[4], rows[5])
    norm3 = norm3.astype(jnp.bfloat16)
    mixed = ff_forward(norm3.reshape(batch * tokens, width), weights['w_ff1'], weights['bias_ff1'][None],
                       weights['w_ff2'])
    residual = residual + mixed.reshape(batch, tokens, width) + rows[8]
    residual = pace(4, residual)
    saved = dict(ln1_back=ln1_back, norm1=norm1, qkv=qkv, self_out=self_out,
                 ln2_back=ln2_back, norm2=norm2, query=query, keys_values=keys_values, cross_out=cross_out,
                 ln3_back=ln3_back, norm3=norm3)
    return residual, saved, weights


def blocks(grad_full):
    return grad_full.astype(jnp.bfloat16).reshape(8, grad_full.shape[0] // 8, grad_full.shape[1])


def launch(tasks, partial, x_first):
    task = Task(scatter_steps(partial, x_first))
    tasks.append(task)
    return task


def block_backward(grad, context, n_keys, weights, saved, tasks, flip):
    batch, tokens, width = grad.shape
    grad_bf = grad.astype(jnp.bfloat16)
    g_bias_ff2 = jnp.sum(grad, axis=(0, 1))
    grad_bf = tick(grad_bf, tasks)
    g_ff1, g_ff2, g_bias_ff1, d_norm = ff_backward(
        saved['norm3'].reshape(batch * tokens, width), grad_bf.reshape(batch * tokens, width),
        weights['w_ff1'], weights['bias_ff1'][None], weights['w_ff2'])
    t_ff2 = launch(tasks, blocks(g_ff2), flip)
    t_ff1 = launch(tasks, g_ff1.reshape(2, 8, width // 8, g_ff1.shape[2]), not flip)
    d_norm = tick(d_norm, tasks)
    d_res, g_ln3_gain, g_ln3_shift = saved['ln3_back'](d_norm.reshape(batch, tokens, width))
    grad = grad + d_res
    grad_bf = grad.astype(jnp.bfloat16)
    g_bias_out2 = jnp.sum(grad, axis=(0, 1))
    g_out2 = weight_grad(saved['cross_out'], grad_bf)
    d_cross = tick(project_back(grad_bf, weights['w_out2']).astype(jnp.bfloat16), tasks)
    d_query, d_kv = cross_attend_back(saved['query'], saved['keys_values'], d_cross, n_keys)
    g_q2 = weight_grad(saved['norm2'], d_query)
    g_kv2 = weight_grad(context, d_kv)
    d_norm = project_back(d_query, weights['w_q2'])
    t_pair = launch(tasks, jnp.concatenate([blocks(g_out2), blocks(g_q2)], axis=1), flip)
    t_kv2 = launch(tasks, blocks(g_kv2), flip)
    d_norm = tick(d_norm, tasks)
    d_res, g_ln2_gain, g_ln2_shift = saved['ln2_back'](d_norm)
    grad = grad + d_res
    grad_bf = grad.astype(jnp.bfloat16)
    g_bias_out = jnp.sum(grad, axis=(0, 1))
    g_out = weight_grad(saved['self_out'], grad_bf)
    d_self = tick(project_back(grad_bf, weights['w_out']).astype(jnp.bfloat16), tasks)
    d_qkv = self_attend_back(saved['qkv'], d_self)
    g_qkv = weight_grad(saved['norm1'], d_qkv)
    t_qkv = launch(tasks, blocks(g_qkv), not flip)
    d_qkv = tick(d_qkv, tasks)
    d_res, g_ln1_gain, g_ln1_shift = saved['ln1_back'](project_back(d_qkv, weights['w_qkv']))
    grad = grad + d_res
    g_vecs = jnp.concatenate([g_ln1_gain, g_ln1_shift, g_ln2_gain, g_ln2_shift, g_ln3_gain, g_ln3_shift,
                              g_bias_out, g_bias_out2, g_bias_ff2, g_bias_ff1.reshape(-1)])
    vec_len = g_vecs.shape[0] // 8
    vec = jnp.pad(g_vecs.reshape(8, vec_len), ((0, 0), (0, VEC_ROWS * width - vec_len)))
    vec = vec.reshape(8, VEC_ROWS, width).astype(jnp.bfloat16)
    t_last = launch(tasks, jnp.concatenate([blocks(g_out), vec], axis=1), flip)
    grad = tick(grad, tasks)

    def collect(total):
        rows = width // 8
        last, pair = t_last.result / total, t_pair.result / total
        return [(t_qkv.result / total).reshape(-1), last[:rows].reshape(-1), pair[rows:].reshape(-1),
                (t_kv2.result / total).reshape(-1), pair[:rows].reshape(-1), jnp.swapaxes(t_ff1.result / total, 0, 1).reshape(-1),
                (t_ff2.result / total).reshape(-1), last[rows:].reshape(-1)[:vec_len]]

    return grad, collect


def solution(mesh):
    n_dev = mesh.shape[AXIS]

    def local(tokens_x, context, cot_out, *shards):
        batch, tokens, width = tokens_x.shape
        ctx_width = context.shape[-1]
        blocks_n = shards[0].shape[0]
        shard_lens = [shard.shape[1] for shard in shards]
        total = batch * n_dev
        n_keys = context.shape[1]
        context = jnp.pad(context, ((0, 0), (0, -n_keys % 128), (0, 0)))
        residual = tokens_x.astype(jnp.float32)
        gathers = [gather_tasks([shard[layer] for shard in shards], width, ctx_width, layer) for layer in range(blocks_n)]
        first, second = gathers
        early = [first['qkv'], first['square']]
        late = [first['kv2'], first['ff1'], first['ff2']]
        for task in early:
            task.advance(task.pending)
        tick((), early + late)
        drain(early)
        after = list(second.values())

        def pace_first(point, chain):
            if point == 0:
                return tick(chain, late)
            if point == 1:
                return tick(chain, late)
            if point == 2:
                return tick(chain, late + after)
            return tick(chain, after)

        def pace_second(point, chain):
            return chain

        residual, saved0, weights0 = block_forward(residual, context, n_keys, first, shard_lens[7], pace_first)
        drain(after)
        residual, saved1, weights1 = block_forward(residual, context, n_keys, second, shard_lens[7], pace_second)
        grad = cot_out.astype(jnp.float32)
        tasks = []
        grad, collect1 = block_backward(grad, context, n_keys, weights1, saved1, tasks, True)
        grad, collect0 = block_backward(grad, context, n_keys, weights0, saved0, tasks, False)
        drain(tasks)
        grad_shards = [collect0(total), collect1(total)]
        stacked = [jnp.stack([per_layer[index] for per_layer in grad_shards]) for index in range(len(shards))]
        return tuple([residual.astype(jnp.bfloat16), grad.astype(jnp.bfloat16)] + stacked)

    param_spec = P(None, AXIS)
    in_specs = (P(AXIS), P(AXIS), P(AXIS)) + (param_spec,) * 8
    out_specs = (P(AXIS), P(AXIS)) + (param_spec,) * 8
    return jax.shard_map(local, mesh=mesh, in_specs=in_specs, out_specs=out_specs, check_vma=False)
```
